32 devices in a mesh: lat: 4 (over y, x), lon: 8 (over z, core).
Axes of the slice: x: 2, y: 2, z: 4, core: 2. Of those that a mesh axis runs over, the one named last changes fastest.
Arguments:
- forcing: float32 [256, 2048], P('lat', 'lon'), may hold values from -32 to 32
- depth_east: float32 [256, 2048], P('lat', 'lon'), may hold values from 0.25 to 4
- depth_north: float32 [256, 2048], P('lat', 'lon'), may hold values from 0.25 to 4
- surface_term: float32 [256, 2048], P('lat', 'lon'), may hold values from 0.02 to 0.5
- ocean_mask: int32 [256, 2048], P('lat', 'lon'), may hold values 0 or 1
- cost_weights: float32 [8, 256, 2048], P(None, 'lat', 'lon'), may hold values from -6 to 6
Outputs:
- forcing_adjoint: float32 [8, 256, 2048], P(None, 'lat', 'lon')
- east_gradient: float32 [8, 256, 2048], P(None, 'lat', 'lon')
- north_gradient: float32 [8, 256, 2048], P(None, 'lat', 'lon')
The draws below stay inside these ranges and needn't reach their ends.
Inputs may be any that keep to these rules, and one draw needn't show every extreme that they name: `ocean_mask`: 1 marks an ocean cell, 0 a land cell.
All inputs are finite; a program needn't handle non-finite values. No bound on the sum of `ocean_mask` on one device may be relied on, other than what follows from the above.
Results may differ from the reference program's by a relative error of at most 0.00018.
Values sent between devices are 32-bit elements; how exact they have to be, the bound alone decides.
A program may use at most 64 MiB of HBM per device.

```python
import math
import jax
import jax.numpy as jnp
from jax import lax

COSTS = 8
ITERS = 6
NLAT = 256
NLON = 2048


def draw_forcing(key, part):
    first = jax.random.fold_in(key, 0)
    rows = jnp.arange(NLAT, dtype=jnp.float32) / NLAT
    cols = jnp.arange(NLON, dtype=jnp.float32) / NLON
    envelope = jnp.exp(jnp.log(3.0) * (0.5 * rows[:, None] + cols[None, :]))
    rough = jnp.clip(jax.random.normal(first, (NLAT, NLON), jnp.float32), -6.0, 6.0)
    return (rough * envelope).astype(jnp.float32)


def plant(values, key, least, high):
    index_at = [jax.random.randint(jax.random.fold_in(key, axis), (), 0, length) for axis, length in enumerate(values.shape)]
    longest = values.shape.index(max(values.shape))
    beside = index_at[:longest] + [(index_at[longest] + 1) % values.shape[longest]] + index_at[longest + 1:]
    return values.at[tuple(index_at)].set(least).at[tuple(beside)].set(high)


def block_scale(own_key, extent, shards, smallest, top_value):
    def one(dim, shards_of):
        heights = jax.random.uniform(jax.random.fold_in(jax.random.fold_in(own_key, 6), dim), (shards_of,), jnp.float32, smallest / len(shards), top_value / len(shards))
        return jnp.repeat(jnp.exp(heights), extent[dim] // shards_of).reshape((-1,) + (1,) * (len(extent) - dim - 1))

    level = one(*shards[0])
    for cut in shards[1:]:
        level = level * one(*cut)
    return level


def scatter_about(key, shape, scale, reach, shards=(), held_as=jnp.bfloat16):
    entries = scale * jax.random.normal(key, shape, jnp.float32)
    if shards:
        entries = entries * block_scale(key, shape, shards, -0.22, 0.18)
    return jnp.clip(entries, -reach, reach).astype(held_as)


def setup_inputs(seed: int = 0) -> dict:
    keys = jax.random.split(jax.random.key(seed), 7)
    forcing = draw_forcing(jax.random.fold_in(keys[6], 71), 0)
    depth_east = jnp.clip(jnp.exp(math.log(4.0) - 2.7725887 * jax.random.uniform(keys[1], (NLAT, NLON), jnp.float32) ** block_scale(keys[1], (NLAT, NLON), ((0, 4), (1, 8)), -0.2, 0.2)), 0.25, 4.0)
    depth_north = jnp.clip(jnp.exp(math.log(4.0) - 2.7725887 * jax.random.uniform(keys[2], (NLAT, NLON), jnp.float32) ** block_scale(keys[2], (NLAT, NLON), ((0, 4), (1, 8)), -0.2, 0.2)), 0.25, 4.0)
    surface_term = jnp.clip(jnp.exp(math.log(0.5) - 3.218876 * jax.random.uniform(keys[3], (NLAT, NLON), jnp.float32) ** block_scale(keys[3], (NLAT, NLON), ((0, 4), (1, 8)), -0.2, 0.2)), 0.02, 0.5)
    ocean_mask = plant((jax.random.randint(keys[4], (NLAT, NLON), 0, 5) < 4).astype(jnp.int32), jax.random.fold_in(keys[4], 1), 0, 1)
    cost_weights = scatter_about(keys[5], (COSTS, NLAT, NLON), 1.0, 6.0, ((1, 4), (2, 8)), jnp.float32)
    return {"forcing": forcing, "depth_east": depth_east, "depth_north": depth_north, "surface_term": surface_term, "ocean_mask": ocean_mask, "cost_weights": cost_weights}


def faces(ocean_mask, depth_east, depth_north, surface_term):
    wet = ocean_mask.astype(jnp.float32)
    wet_east = jnp.roll(wet, -1, axis=1)
    wet_north = jnp.concatenate([wet[1:], jnp.zeros((1, wet.shape[1]), jnp.float32)], axis=0)
    east_face = depth_east * wet * wet_east
    north_face = depth_north * wet * wet_north
    west_face = jnp.roll(east_face, 1, axis=1)
    south_face = jnp.concatenate([jnp.zeros((1, wet.shape[1]), jnp.float32), north_face[:-1]], axis=0)
    base = wet * surface_term + 1.0 - wet
    return (base, east_face, west_face, north_face, south_face)

def operate(field, coefs):
    base, east_face, west_face, north_face, south_face = coefs
    east = jnp.roll(field, -1, axis=1)
    west = jnp.roll(field, 1, axis=1)
    zero_row = jnp.zeros((1, field.shape[1]), jnp.float32)
    north = jnp.concatenate([field[1:], zero_row], axis=0)
    south = jnp.concatenate([zero_row, field[:-1]], axis=0)
    return base * field + east_face * (field - east) + west_face * (field - west) + north_face * (field - north) + south_face * (field - south)

def solve(forcing, depth_east, depth_north, surface_term, ocean_mask):
    coefs = faces(ocean_mask, depth_east, depth_north, surface_term)
    diagonal = coefs[0] + coefs[1] + coefs[2] + coefs[3] + coefs[4]
    iterate = jnp.zeros_like(forcing)
    residual = forcing
    precond = residual / diagonal
    direction = precond
    norm_now = jnp.sum(residual * precond)
    for step in range(ITERS):
        image = operate(direction, coefs)
        alpha = norm_now / jnp.sum(direction * image)
        iterate = iterate + alpha * direction
        residual = residual - alpha * image
        if step < ITERS - 1:
            precond = residual / diagonal
            norm_next = jnp.sum(residual * precond)
            direction = precond + norm_next / norm_now * direction
            norm_now = norm_next
    return iterate

def reference(forcing, depth_east, depth_north, surface_term, ocean_mask, cost_weights):

    def forward(rhs_field, east_depth, north_depth):
        return solve(rhs_field, east_depth, north_depth, surface_term, ocean_mask)
    _, pullback = jax.vjp(forward, forcing, depth_east, depth_north)
    grads = lax.map(lambda weight: pullback(weight), cost_weights)
    return (grads[0], grads[1], grads[2])
```

```python
import functools

import jax
import jax.numpy as jnp
from jax import lax
from jax.experimental import pallas as pl
from jax.experimental.pallas import tpu as pltpu
from jax.sharding import PartitionSpec as P

ITERS = 6
MESH = pl.DeviceIdType.MESH
HR = 16
HB = 8
HC = 13
HW = 6


def cost_of(mu, proj):
    def dot(a, b):
        acc = [None] * (len(a) + len(b) - 1)
        for i, x in enumerate(a):
            for j, y in enumerate(b):
                if a is b and j < i:
                    continue
                pr = x * y
                if a is b and j > i:
                    pr = pr + pr
                for m in (i + j, abs(i - j)):
                    acc[m] = pr if acc[m] is None else acc[m] + pr
        tot = acc[0] * mu[0]
        for m in range(1, len(acc)):
            tot = tot + acc[m] * mu[m]
        return 0.5 * tot

    def apply(p):
        q = list(p) + [None]
        for k, x in enumerate(p):
            if k == 0:
                q[1] = -x if q[1] is None else q[1] - x
            else:
                hx = 0.5 * x
                q[k + 1] = -hx if q[k + 1] is None else q[k + 1] - hx
                q[k - 1] = q[k - 1] - hx
        return q

    one = jnp.ones_like(mu[0])
    z, p, rz, cost = [one], [one], mu[0], None
    for step in range(ITERS):
        q = apply(p)
        alpha = rz / dot(p, q)
        term = p[0] * proj[0]
        for k in range(1, len(p)):
            term = term + p[k] * proj[k]
        cost = alpha * term if cost is None else cost + alpha * term
        if step < ITERS - 1:
            z = [z[k] - alpha * q[k] for k in range(len(z))] + [-alpha * q[-1]]
            rz_new = dot(z, z)
            beta = rz_new / rz
            p = [z[k] + beta * p[k] for k in range(len(p))] + [z[-1]]
            rz = rz_new
    return cost


def roll(x, shift, axis):
    return pltpu.roll(x, shift % x.shape[axis], axis)


def east(x):
    return roll(x, -1, 1)


def north(x):
    return roll(x, -1, 0)


def kernel(nlat, nlon, names, f_ref, de_ref, dn_ref, st_ref, mk_ref, w_ref, fa_ref, ge_ref, gn_ref,
           send_w, send_e, recv_e, recv_w, row_n, row_s, mrow_n, mrow_s, wrow_n, wrow_s,
           part, part2, got_lon, got_lat, sums, wp, coef,
           ssem, rsem, ss_lon, rs_lon, ss_lat, rs_lat):
    lat, lon = lax.axis_index("lat"), lax.axis_index("lon")
    costs, rows, cols = w_ref.shape

    def peer(dlat, dlon):
        return (lax.rem(lat + dlat + nlat, nlat), lax.rem(lon + dlon + nlon, nlon))

    peers = {(a % nlat, b % nlon) for a in (-1, 0, 1) for b in (-1, 0, 1)}
    peers |= {(0, b) for b in range(nlon)} | {(a, 0) for a in range(nlat)}
    peers = sorted(peers - {(0, 0)})
    barrier = pltpu.get_barrier_semaphore()
    for a, b in peers:
        pl.semaphore_signal(barrier, inc=1, device_id=peer(a, b), device_id_type=MESH)

    lane = lax.broadcasted_iota(jnp.int32, (rows, 128), 1)
    wide = [f_ref, de_ref, dn_ref, st_ref, mk_ref]
    for ref, at, first in ((send_w, slice(0, 128), True), (send_e, slice(cols - 128, cols), False)):
        buf = jnp.zeros((rows, 128), jnp.float32)
        pos = 0
        for i in range(5 + costs):
            width = HC if i < 5 else HW
            tile = (wide[i][:, at] if i < 5 else w_ref[i - 5, :, at]).astype(jnp.float32)
            tile = roll(tile, pos if first else pos + width, 1)
            buf = jnp.where((lane >= pos) & (lane < pos + width), tile, buf)
            pos += width
        ref[...] = buf
    pl.semaphore_wait(barrier, len(peers))

    copies = []

    def send(src, dst, dev):
        i = len(copies)
        c = pltpu.make_async_remote_copy(src_ref=src, dst_ref=dst, send_sem=ssem.at[i],
                                         recv_sem=rsem.at[i], device_id=dev, device_id_type=MESH)
        c.start()
        copies.append(c)

    lo, hi = pl.ds(0, HR), pl.ds(rows - HR, HR)
    for src, dst, d in ((send_w, recv_e, -1), (send_e, recv_w, 1)):
        send(src.at[lo], dst.at[pl.ds(rows, HR)], peer(-1, d))
        send(src.at[hi], dst.at[pl.ds(rows + HR, HR)], peer(1, d))
        send(src, dst.at[pl.ds(0, rows)], peer(0, d))
    for i in range(5):
        src = wide[i]
        send(src.at[lo], row_n.at[i] if i < 4 else mrow_n, peer(-1, 0))
        send(src.at[hi], row_s.at[i] if i < 4 else mrow_s, peer(1, 0))
    early = len(copies)
    send(w_ref.at[:, pl.ds(0, HB)], wrow_n, peer(-1, 0))
    send(w_ref.at[:, pl.ds(rows - HB, HB)], wrow_s, peer(1, 0))
    for c in copies[:early]:
        c.wait_recv()

    full = rows + 2 * HR
    lane = lax.broadcasted_iota(jnp.int32, (full, 128), 1)
    got_e, got_w = recv_e[...], recv_w[...]

    def side(pos, width):
        a = roll(got_e, -pos, 1)
        b = roll(got_w, 128 - width - pos, 1)
        return jnp.where(lane < width, a, jnp.where(lane >= 128 - width, b, 0.0))

    def padded(i):
        if i < 4:
            top, mid, low = row_n[i], wide[i][...], row_s[i]
        else:
            top, mid, low = (r[...].astype(jnp.float32) for r in (mrow_n, mk_ref, mrow_s))
        return jnp.concatenate([jnp.concatenate([mid, top, low], axis=0), side(HC * i, HC)], axis=1)

    ringc = cols + 128
    row_id = lax.broadcasted_iota(jnp.int32, (full, ringc), 0)
    keep_n = (lat < nlat - 1).astype(jnp.float32)
    keep_s = (lat > 0).astype(jnp.float32)
    edge = jnp.where(row_id < rows, 1.0, jnp.where(row_id < rows + HR, keep_n, keep_s))
    wet = padded(4) * edge
    ex = padded(1) * wet * east(wet)
    ey = padded(2) * wet * north(wet)
    base = wet * padded(3) + 1.0 - wet
    diag = base + ex + roll(ex, 1, 1) + ey + roll(ey, 1, 0)
    rs = lax.rsqrt(diag)
    rs = rs * (1.5 - 0.5 * diag * rs * rs)
    rs_e, rs_n = rs * east(rs), rs * north(rs)
    e2 = 2.0 * ex * rs_e
    n2 = 2.0 * ey * rs_n

    def twice(v, e2, n2):
        return e2 * east(v) + roll(e2 * v, 1, 1) + n2 * north(v) + roll(n2 * v, 1, 0)

    us = [rs * padded(0)]
    us.append(0.5 * twice(us[0], e2, n2))
    for k in range(1, ITERS):
        us.append(twice(us[k], e2, n2) - us[k - 1])

    inner = [u[:rows, :cols] for u in us]
    rs_in = rs[:rows, :cols]

    def put(at, field):
        line = jnp.sum(field, axis=0, keepdims=True)
        tot = line[:, :128]
        for c in range(128, cols, 128):
            tot = tot + line[:, c:c + 128]
        sums[at:at + 1, :] = tot

    sums[...] = jnp.zeros_like(sums)
    mom = ITERS * costs
    for k in range(ITERS):
        put(mom + 2 * k, inner[k] * inner[k])
        put(mom + 2 * k + 1, inner[k] * inner[k + 1])
    for n in range(costs):
        wn = w_ref[n] * rs_in
        for k in range(ITERS):
            put(k * costs + n, wn * inner[k])
    nsum = sums.shape[0]
    lane_s = lax.broadcasted_iota(jnp.int32, (nsum, 128), 1)
    row_s_id = lax.broadcasted_iota(jnp.int32, (nsum, 128), 0)
    by_row = jnp.sum(sums[...], axis=1, keepdims=True)
    mine = jnp.sum(jnp.where(lane_s == row_s_id, by_row, 0.0), axis=0, keepdims=True)
    part[...] = mine
    lon_copies = []
    for d in range(1, nlon):
        c = pltpu.make_async_remote_copy(src_ref=part, dst_ref=got_lon.at[d - 1],
                                         send_sem=ss_lon.at[d - 1], recv_sem=rs_lon.at[d - 1],
                                         device_id=peer(0, d), device_id_type=MESH)
        c.start()
        lon_copies.append(c)

    for c in copies[early:]:
        c.wait_recv()

    def cut(x):
        return jnp.concatenate([x[:rows + HB], x[full - HB:]], axis=0)

    rs_b = cut(rs)
    for n in range(costs):
        block = jnp.concatenate([w_ref[n], wrow_n[n], wrow_s[n]], axis=0)
        tile = cut(side(5 * HC + HW * n, HW))
        wp[n] = rs_b * jnp.concatenate([block, tile], axis=1)
    e2b, n2b = cut(e2), cut(n2)
    ub = [cut(u) for u in us]

    for c in lon_copies:
        c.wait_recv()
    total = mine
    for d in range(1, nlon):
        total = total + got_lon[d - 1]
    part2[...] = total
    lat_copies = []
    for d in range(1, nlat):
        c = pltpu.make_async_remote_copy(src_ref=part2, dst_ref=got_lat.at[d - 1],
                                         send_sem=ss_lat.at[d - 1], recv_sem=rs_lat.at[d - 1],
                                         device_id=peer(d, 0), device_id_type=MESH)
        c.start()
        lat_copies.append(c)
    for c in lat_copies:
        c.wait_recv()
    for d in range(1, nlat):
        total = total + got_lat[d - 1]

    tot8 = jnp.broadcast_to(total, (costs, 128))
    lane8 = lax.broadcasted_iota(jnp.int32, (costs, 128), 1)
    sub8 = lax.broadcasted_iota(jnp.int32, (costs, 128), 0)

    def pick(index):
        return jnp.broadcast_to(
            jnp.sum(jnp.where(lane8 == index, tot8, 0.0), axis=1, keepdims=True), (costs, 128))

    proj = [pick(k * costs + sub8) for k in range(ITERS)]
    raw = [pick(mom + m) for m in range(2 * ITERS)]
    mu = [raw[0], raw[1]]
    for k in range(1, ITERS):
        mu += [2.0 * raw[2 * k] - raw[0], 2.0 * raw[2 * k + 1] - raw[1]]
    cost, pull = jax.vjp(cost_of, mu, proj)
    mu_bar, x = pull(jnp.ones_like(cost))
    even = [2.0 * mu_bar[2 * k] for k in range(ITERS)]
    odd = [2.0 * mu_bar[2 * k + 1] for k in range(ITERS)]
    even[0] = mu_bar[0] - 0.5 * sum(even[1:])
    odd[0] = mu_bar[1] - 0.5 * sum(odd[1:])
    reps = ringc // 128
    for k in range(ITERS):
        for i, v in enumerate((x[k], 2.0 * even[k], odd[k])):
            coef[3 * k + i] = jnp.concatenate([v] * reps, axis=1)

    u_half = [0.5 * u for u in ub]
    ug = [u_half[0]] + ub[1:]
    u_in = [u[:rows, :cols] for u in ug]
    u_east = [east(u)[:rows, :cols] for u in ug]
    u_north = [north(u)[:rows, :cols] for u in ug]
    quad = [ub[0], ub[1]] + [ub[k] + ub[k - 2] for k in range(2, ITERS)] + [u_half[6] + ub[4]]
    wet_in = wet[:rows, :cols]
    me = wet_in * east(wet)[:rows, :cols]
    mn = wet_in * north(wet)[:rows, :cols]
    mre = 2.0 * me * rs_e[:rows, :cols]
    mrn = 2.0 * mn * rs_n[:rows, :cols]
    neg = -(rs_b * rs_b)

    def one(n, carry):
        def c(i):
            return coef[i, pl.ds(n, 1), :]

        wn = wp[n]
        nxt = c(3 * 5 + 2) * ub[5]
        nxt2 = None
        dd = nxt * quad[6]
        eb = nb = None
        for k in range(ITERS - 1, -1, -1):
            le, ln = east(nxt), north(nxt)
            s2 = e2b * le + roll(e2b * nxt, 1, 1) + n2b * ln + roll(n2b * nxt, 1, 0)
            if k == 0:
                s2 = 0.5 * s2
            lin = nxt[:rows, :cols]
            ea = lin * u_east[k] + le[:rows, :cols] * u_in[k]
            na = lin * u_north[k] + ln[:rows, :cols] * u_in[k]
            eb = ea if eb is None else eb + ea
            nb = na if nb is None else nb + na
            seed = c(3 * k + 1) * ub[k] + c(3 * k + 2) * ub[k + 1]
            if k > 0:
                seed = seed + c(3 * k - 1) * ub[k - 1]
            lam = c(3 * k) * wn + seed + s2
            if nxt2 is not None:
                lam = lam - nxt2
            dd = dd + lam * quad[k] - seed * u_half[k]
            nxt, nxt2 = lam, nxt
        fa_ref[n] = rs_in * nxt[:rows, :cols]
        db = neg * dd
        db_in = db[:rows, :cols]
        ge_ref[n] = mre * eb + me * (db_in + east(db)[:rows, :cols])
        gn_ref[n] = mrn * nb + mn * (db_in + north(db)[:rows, :cols])
        return carry

    lax.fori_loop(0, costs, one, 0)
    for c in copies + lon_copies + lat_copies:
        c.wait_send()


def solution(mesh):
    nlat, nlon = mesh.shape["lat"], mesh.shape["lon"]

    def body(forcing, depth_east, depth_north, surface_term, ocean_mask, cost_weights):
        costs, rows, cols = cost_weights.shape
        full, ringc = rows + 2 * HR, cols + 128
        f32 = jnp.float32
        dma = pltpu.SemaphoreType.DMA
        nsum = -(-(ITERS * costs + 2 * ITERS) // 8) * 8
        vmem = pl.BlockSpec(memory_space=pltpu.VMEM)
        return pl.pallas_call(
            functools.partial(kernel, nlat, nlon, None),
            out_shape=[jax.ShapeDtypeStruct((costs, rows, cols), f32)] * 3,
            in_specs=[vmem] * 6,
            out_specs=[vmem] * 3,
            scratch_shapes=[
                pltpu.VMEM((rows, 128), f32),
                pltpu.VMEM((rows, 128), f32),
                pltpu.VMEM((full, 128), f32),
                pltpu.VMEM((full, 128), f32),
                pltpu.VMEM((4, HR, cols), f32),
                pltpu.VMEM((4, HR, cols), f32),
                pltpu.VMEM((HR, cols), jnp.int32),
                pltpu.VMEM((HR, cols), jnp.int32),
                pltpu.VMEM((costs, HB, cols), f32),
                pltpu.VMEM((costs, HB, cols), f32),
                pltpu.VMEM((1, 128), f32),
                pltpu.VMEM((1, 128), f32),
                pltpu.VMEM((nlon - 1, 1, 128), f32),
                pltpu.VMEM((nlat - 1, 1, 128), f32),
                pltpu.VMEM((nsum, 128), f32),
                pltpu.VMEM((costs, rows + 2 * HB, ringc), f32),
                pltpu.VMEM((3 * ITERS, costs, ringc), f32),
                dma((18,)),
                dma((18,)),
                dma((nlon - 1,)),
                dma((nlon - 1,)),
                dma((nlat - 1,)),
                dma((nlat - 1,)),
            ],
            compiler_params=pltpu.CompilerParams(
                collective_id=0, has_side_effects=True, vmem_limit_bytes=48 * 1024 * 1024
            ),
        )(forcing, depth_east, depth_north, surface_term, ocean_mask, cost_weights)

    grid = P("lat", "lon")
    field = P(None, "lat", "lon")
    return jax.shard_map(
        body,
        mesh=mesh,
        in_specs=(grid, grid, grid, grid, grid, field),
        out_specs=(field, field, field),
        check_vma=False,
    )
```

```python
import functools

import jax
import jax.numpy as jnp
from jax import lax
from jax.experimental import pallas as pl
from jax.experimental.pallas import tpu as pltpu
from jax.sharding import PartitionSpec as P

ITERS = 6
MESH = pl.DeviceIdType.MESH
HR = 16
HB = 8
HC = 13
HW = 6


def cost_of(mu, proj):
    def dot(a, b):
        acc = [None] * (len(a) + len(b) - 1)
        for i, x in enumerate(a):
            for j, y in enumerate(b):
                if a is b and j < i:
                    continue
                pr = x * y
                if a is b and j > i:
                    pr = pr + pr
                for m in (i + j, abs(i - j)):
                    acc[m] = pr if acc[m] is None else acc[m] + pr
        tot = acc[0] * mu[0]
        for m in range(1, len(acc)):
            tot = tot + acc[m] * mu[m]
        return 0.5 * tot

    def apply(p):
        q = list(p) + [None]
        for k, x in enumerate(p):
            if k == 0:
                q[1] = -x if q[1] is None else q[1] - x
            else:
                hx = 0.5 * x
                q[k + 1] = -hx if q[k + 1] is None else q[k + 1] - hx
                q[k - 1] = q[k - 1] - hx
        return q

    one = jnp.ones_like(mu[0])
    z, p, rz, cost = [one], [one], mu[0], None
    for step in range(ITERS):
        q = apply(p)
        alpha = rz / dot(p, q)
        term = p[0] * proj[0]
        for k in range(1, len(p)):
            term = term + p[k] * proj[k]
        cost = alpha * term if cost is None else cost + alpha * term
        if step < ITERS - 1:
            z = [z[k] - alpha * q[k] for k in range(len(z))] + [-alpha * q[-1]]
            rz_new = dot(z, z)
            beta = rz_new / rz
            p = [z[k] + beta * p[k] for k in range(len(p))] + [z[-1]]
            rz = rz_new
    return cost


def roll(x, shift, axis):
    return pltpu.roll(x, shift % x.shape[axis], axis)


def east(x):
    return roll(x, -1, 1)


def north(x):
    return roll(x, -1, 0)


def kernel(nlat, nlon, stages, f_hbm, de_hbm, dn_hbm, st_hbm, mk_hbm, w_hbm, fa_ref, ge_ref, gn_ref,
           f_ref, de_ref, dn_ref, st_ref, mk_ref, w_ref, lsem,
           send_w, send_e, recv_e, recv_w, row_n, row_s, mrow_n, mrow_s, wrow_n, wrow_s,
           sums, wp, coef, ssem, rsem, *reduce_refs):
    lat, lon = lax.axis_index("lat"), lax.axis_index("lon")
    costs, rows, cols = w_ref.shape
    loads = [pltpu.make_async_copy(src, dst, lsem.at[i]) for i, (src, dst) in enumerate(
        zip((f_hbm, de_hbm, dn_hbm, st_hbm, mk_hbm, w_hbm),
            (f_ref, de_ref, dn_ref, st_ref, mk_ref, w_ref)))]
    for c in loads:
        c.start()

    def peer(dlat, dlon):
        return (lax.rem(lat + dlat + nlat, nlat), lax.rem(lon + dlon + nlon, nlon))

    peers = {(a % nlat, b % nlon) for a in (-1, 0, 1) for b in (-1, 0, 1)}
    peers |= {o for stage in stages for o in stage}
    peers = sorted(peers - {(0, 0)})
    barrier = pltpu.get_barrier_semaphore()
    for a, b in peers:
        pl.semaphore_signal(barrier, inc=1, device_id=peer(a, b), device_id_type=MESH)

    for c in loads:
        c.wait()

    lane = lax.broadcasted_iota(jnp.int32, (rows, 128), 1)
    wide = [f_ref, de_ref, dn_ref, st_ref, mk_ref]
    for ref, at, first in ((send_w, slice(0, 128), True), (send_e, slice(cols - 128, cols), False)):
        buf = jnp.zeros((rows, 128), jnp.float32)
        pos = 0
        for i in range(5 + costs):
            width = HC if i < 5 else HW
            tile = (wide[i][:, at] if i < 5 else w_ref[i - 5, :, at]).astype(jnp.float32)
            tile = roll(tile, pos if first else pos + width, 1)
            buf = jnp.where((lane >= pos) & (lane < pos + width), tile, buf)
            pos += width
        ref[...] = buf
    pl.semaphore_wait(barrier, len(peers))

    copies = []

    def send(src, dst, dev):
        i = len(copies)
        c = pltpu.make_async_remote_copy(src_ref=src, dst_ref=dst, send_sem=ssem.at[i],
                                         recv_sem=rsem.at[i], device_id=dev, device_id_type=MESH)
        c.start()
        copies.append(c)

    lo, hi = pl.ds(0, HR), pl.ds(rows - HR, HR)
    for src, dst, d in ((send_w, recv_e, -1), (send_e, recv_w, 1)):
        send(src.at[lo], dst.at[pl.ds(rows, HR)], peer(-1, d))
        send(src.at[hi], dst.at[pl.ds(rows + HR, HR)], peer(1, d))
        send(src, dst.at[pl.ds(0, rows)], peer(0, d))
    for i in range(5):
        src = wide[i]
        send(src.at[lo], row_n.at[i] if i < 4 else mrow_n, peer(-1, 0))
        send(src.at[hi], row_s.at[i] if i < 4 else mrow_s, peer(1, 0))
    early = len(copies)
    send(w_ref.at[:, pl.ds(0, HB)], wrow_n, peer(-1, 0))
    send(w_ref.at[:, pl.ds(rows - HB, HB)], wrow_s, peer(1, 0))
    for c in copies[:early]:
        c.wait_recv()

    full = rows + 2 * HR
    lane = lax.broadcasted_iota(jnp.int32, (full, 128), 1)
    got_e, got_w = recv_e[...], recv_w[...]

    def side(pos, width):
        a = roll(got_e, -pos, 1)
        b = roll(got_w, 128 - width - pos, 1)
        return jnp.where(lane < width, a, jnp.where(lane >= 128 - width, b, 0.0))

    def padded(i):
        if i < 4:
            top, mid, low = row_n[i], wide[i][...], row_s[i]
        else:
            top, mid, low = (r[...].astype(jnp.float32) for r in (mrow_n, mk_ref, mrow_s))
        return jnp.concatenate([jnp.concatenate([mid, top, low], axis=0), side(HC * i, HC)], axis=1)

    ringc = cols + 128
    row_id = lax.broadcasted_iota(jnp.int32, (full, ringc), 0)
    keep_n = (lat < nlat - 1).astype(jnp.float32)
    keep_s = (lat > 0).astype(jnp.float32)
    edge = jnp.where(row_id < rows, 1.0, jnp.where(row_id < rows + HR, keep_n, keep_s))
    wet = padded(4) * edge
    ex = padded(1) * wet * east(wet)
    ey = padded(2) * wet * north(wet)
    base = wet * padded(3) + 1.0 - wet
    diag = base + ex + roll(ex, 1, 1) + ey + roll(ey, 1, 0)
    rs = lax.rsqrt(diag)
    rs = rs * (1.5 - 0.5 * diag * rs * rs)
    rs_e, rs_n = rs * east(rs), rs * north(rs)
    e2 = 2.0 * ex * rs_e
    n2 = 2.0 * ey * rs_n

    def twice(v, e2, n2):
        return e2 * east(v) + roll(e2 * v, 1, 1) + n2 * north(v) + roll(n2 * v, 1, 0)

    us = [rs * padded(0)]
    us.append(0.5 * twice(us[0], e2, n2))
    for k in range(1, ITERS):
        us.append(twice(us[k], e2, n2) - us[k - 1])

    inner = [u[:rows, :cols] for u in us]
    rs_in = rs[:rows, :cols]

    def put(at, field):
        line = jnp.sum(field, axis=0, keepdims=True)
        tot = line[:, :128]
        for c in range(128, cols, 128):
            tot = tot + line[:, c:c + 128]
        sums[at:at + 1, :] = tot

    sums[...] = jnp.zeros_like(sums)
    mom = ITERS * costs
    for k in range(ITERS):
        put(mom + 2 * k, inner[k] * inner[k])
        put(mom + 2 * k + 1, inner[k] * inner[k + 1])
    for n in range(costs):
        wn = w_ref[n] * rs_in
        for k in range(ITERS):
            put(k * costs + n, wn * inner[k])
    nsum = sums.shape[0]
    lane_s = lax.broadcasted_iota(jnp.int32, (nsum, 128), 1)
    row_s_id = lax.broadcasted_iota(jnp.int32, (nsum, 128), 0)
    by_row = jnp.sum(sums[...], axis=1, keepdims=True)
    mine = jnp.sum(jnp.where(lane_s == row_s_id, by_row, 0.0), axis=0, keepdims=True)
    reduce_copies = []

    def start(stage, value):
        mailbox, got, ss, rv = reduce_refs[4 * stage:4 * stage + 4]
        mailbox[...] = value
        group = []
        for i, (a, b) in enumerate(stages[stage]):
            c = pltpu.make_async_remote_copy(src_ref=mailbox, dst_ref=got.at[i], send_sem=ss.at[i],
                                             recv_sem=rv.at[i], device_id=peer(a, b),
                                             device_id_type=MESH)
            c.start()
            group.append(c)
        reduce_copies.extend(group)
        return group

    def finish(stage, group, value):
        for c in group:
            c.wait_recv()
        for i in range(len(group)):
            value = value + reduce_refs[4 * stage + 1][i]
        return value

    group = start(0, mine)

    for c in copies[early:]:
        c.wait_recv()

    def cut(x):
        return jnp.concatenate([x[:rows + HB], x[full - HB:]], axis=0)

    rs_b = cut(rs)
    for n in range(costs):
        block = jnp.concatenate([w_ref[n], wrow_n[n], wrow_s[n]], axis=0)
        tile = cut(side(5 * HC + HW * n, HW))
        wp[n] = rs_b * jnp.concatenate([block, tile], axis=1)
    e2b, n2b = cut(e2), cut(n2)
    ub = [cut(u) for u in us]

    ug = [0.5 * ub[0]] + ub[1:]
    u_in = [u[:rows, :cols] for u in ug]
    u_east = [east(u)[:rows, :cols] for u in ug]
    u_north = [north(u)[:rows, :cols] for u in ug]
    quad = [ub[0], ub[1]] + [ub[k] + ub[k - 2] for k in range(2, ITERS)] + [0.5 * ub[6] + ub[4]]
    wet_in = wet[:rows, :cols]
    me = wet_in * east(wet)[:rows, :cols]
    mn = wet_in * north(wet)[:rows, :cols]
    mre = 2.0 * me * rs_e[:rows, :cols]
    mrn = 2.0 * mn * rs_n[:rows, :cols]
    neg = -(rs_b * rs_b)

    total = finish(0, group, mine)
    for stage in range(1, len(stages)):
        total = finish(stage, start(stage, total), total)

    tot8 = jnp.broadcast_to(total, (costs, 128))
    lane8 = lax.broadcasted_iota(jnp.int32, (costs, 128), 1)
    sub8 = lax.broadcasted_iota(jnp.int32, (costs, 128), 0)

    def pick(index):
        return jnp.broadcast_to(
            jnp.sum(jnp.where(lane8 == index, tot8, 0.0), axis=1, keepdims=True), (costs, 128))

    proj = [pick(k * costs + sub8) for k in range(ITERS)]
    raw = [pick(mom + m) for m in range(2 * ITERS)]
    mu = [raw[0], raw[1]]
    for k in range(1, ITERS):
        mu += [2.0 * raw[2 * k] - raw[0], 2.0 * raw[2 * k + 1] - raw[1]]
    cost, pull = jax.vjp(cost_of, mu, proj)
    mu_bar, x = pull(jnp.ones_like(cost))
    even = [2.0 * mu_bar[2 * k] for k in range(ITERS)]
    odd = [2.0 * mu_bar[2 * k + 1] for k in range(ITERS)]
    even[0] = mu_bar[0] - 0.5 * sum(even[1:])
    odd[0] = mu_bar[1] - 0.5 * sum(odd[1:])
    reps = ringc // 128
    for k in range(ITERS):
        for i, v in enumerate((x[k], 2.0 * even[k], odd[k])):
            coef[3 * k + i] = jnp.concatenate([v] * reps, axis=1)

    def one(n, carry):
        def c(i):
            return coef[i, pl.ds(n, 1), :]

        wn = wp[n]
        nxt = c(3 * 5 + 2) * ub[5]
        nxt2 = None
        dd = nxt * quad[6]
        eb = nb = du = None
        for k in range(ITERS - 1, -1, -1):
            le, ln = east(nxt), north(nxt)
            s2 = e2b * le + roll(e2b * nxt, 1, 1) + n2b * ln + roll(n2b * nxt, 1, 0)
            if k == 0:
                s2 = 0.5 * s2
            lin = nxt[:rows, :cols]
            ea = lin * u_east[k] + le[:rows, :cols] * u_in[k]
            na = lin * u_north[k] + ln[:rows, :cols] * u_in[k]
            eb = ea if eb is None else eb + ea
            nb = na if nb is None else nb + na
            seed = c(3 * k + 1) * ub[k] + c(3 * k + 2) * ub[k + 1]
            if k > 0:
                seed = seed + c(3 * k - 1) * ub[k - 1]
            lam = c(3 * k) * wn + seed + s2
            if nxt2 is not None:
                lam = lam - nxt2
            dd = dd + lam * quad[k]
            du = seed * ub[k] if du is None else du + seed * ub[k]
            nxt, nxt2 = lam, nxt
        fa_ref[n] = rs_in * nxt[:rows, :cols]
        db = neg * (dd - 0.5 * du)
        db_in = db[:rows, :cols]
        ge_ref[n] = mre * eb + me * (db_in + east(db)[:rows, :cols])
        gn_ref[n] = mrn * nb + mn * (db_in + north(db)[:rows, :cols])
        return carry

    lax.fori_loop(0, costs, one, 0)
    for c in copies + reduce_copies:
        c.wait_send()


def solution(mesh):
    nlat, nlon = mesh.shape["lat"], mesh.shape["lon"]

    def body(forcing, depth_east, depth_north, surface_term, ocean_mask, cost_weights):
        costs, rows, cols = cost_weights.shape
        full, ringc = rows + 2 * HR, cols + 128
        f32 = jnp.float32
        dma = pltpu.SemaphoreType.DMA
        nsum = -(-(ITERS * costs + 2 * ITERS) // 8) * 8
        every = [(a, b) for a in range(nlat) for b in range(nlon) if a or b]
        stages = [every] if len(every) < 64 else [
            [(0, b) for b in range(1, nlon)], [(a, 0) for a in range(1, nlat)]]
        reduce_scratch = [
            ref for g in stages for ref in (
                pltpu.VMEM((1, 128), f32), pltpu.VMEM((len(g), 1, 128), f32),
                dma((len(g),)), dma((len(g),)))]
        vmem = pl.BlockSpec(memory_space=pltpu.VMEM)
        return pl.pallas_call(
            functools.partial(kernel, nlat, nlon, stages),
            out_shape=[jax.ShapeDtypeStruct((costs, rows, cols), f32)] * 3,
            in_specs=[pl.BlockSpec(memory_space=pltpu.HBM)] * 6,
            out_specs=[vmem] * 3,
            scratch_shapes=[
                *[pltpu.VMEM((rows, cols), f32)] * 4,
                pltpu.VMEM((rows, cols), jnp.int32),
                pltpu.VMEM((costs, rows, cols), f32),
                dma((6,)),
                pltpu.VMEM((rows, 128), f32),
                pltpu.VMEM((rows, 128), f32),
                pltpu.VMEM((full, 128), f32),
                pltpu.VMEM((full, 128), f32),
                pltpu.VMEM((4, HR, cols), f32),
                pltpu.VMEM((4, HR, cols), f32),
                pltpu.VMEM((HR, cols), jnp.int32),
                pltpu.VMEM((HR, cols), jnp.int32),
                pltpu.VMEM((costs, HB, cols), f32),
                pltpu.VMEM((costs, HB, cols), f32),
                pltpu.VMEM((nsum, 128), f32),
                pltpu.VMEM((costs, rows + 2 * HB, ringc), f32),
                pltpu.VMEM((3 * ITERS, costs, ringc), f32),
                dma((18,)),
                dma((18,)),
                *reduce_scratch,
            ],
            compiler_params=pltpu.CompilerParams(
                collective_id=0, has_side_effects=True, vmem_limit_bytes=63 * 1024 * 1024
            ),
        )(forcing, depth_east, depth_north, surface_term, ocean_mask, cost_weights)

    grid = P("lat", "lon")
    field = P(None, "lat", "lon")
    return jax.shard_map(
        body,
        mesh=mesh,
        in_specs=(grid, grid, grid, grid, grid, field),
        out_specs=(field, field, field),
        check_vma=False,
    )
```

```python
import functools

import jax
import jax.numpy as jnp
from jax import lax
from jax.experimental import pallas as pl
from jax.experimental.pallas import tpu as pltpu
from jax.sharding import PartitionSpec as P

ITERS = 6
MESH = pl.DeviceIdType.MESH
HR = 16
HB = 8
HC = 13
HW = 6


def cost_of(mu, proj):
    def dot(a, b):
        acc = [None] * (len(a) + len(b) - 1)
        for i, x in enumerate(a):
            for j, y in enumerate(b):
                if a is b and j < i:
                    continue
                pr = x * y
                if a is b and j > i:
                    pr = pr + pr
                for m in (i + j, abs(i - j)):
                    acc[m] = pr if acc[m] is None else acc[m] + pr
        tot = acc[0] * mu[0]
        for m in range(1, len(acc)):
            tot = tot + acc[m] * mu[m]
        return 0.5 * tot

    def apply(p):
        q = list(p) + [None]
        for k, x in enumerate(p):
            if k == 0:
                q[1] = -x if q[1] is None else q[1] - x
            else:
                hx = 0.5 * x
                q[k + 1] = -hx if q[k + 1] is None else q[k + 1] - hx
                q[k - 1] = q[k - 1] - hx
        return q

    one = jnp.ones_like(mu[0])
    z, p, rz, cost = [one], [one], mu[0], None
    for step in range(ITERS):
        q = apply(p)
        alpha = rz / dot(p, q)
        term = p[0] * proj[0]
        for k in range(1, len(p)):
            term = term + p[k] * proj[k]
        cost = alpha * term if cost is None else cost + alpha * term
        if step < ITERS - 1:
            z = [z[k] - alpha * q[k] for k in range(len(z))] + [-alpha * q[-1]]
            rz_new = dot(z, z)
            beta = rz_new / rz
            p = [z[k] + beta * p[k] for k in range(len(p))] + [z[-1]]
            rz = rz_new
    return cost


def roll(x, shift, axis):
    return pltpu.roll(x, shift % x.shape[axis], axis)


def east(x):
    return roll(x, -1, 1)


def north(x):
    return roll(x, -1, 0)


def kernel(nlat, nlon, stages, f_hbm, de_hbm, dn_hbm, st_hbm, mk_hbm, w_hbm, wp_out, pack_out, geo_out, coef_out,
           f_ref, de_ref, dn_ref, st_ref, mk_ref, w_ref, lsem,
           send_w, send_e, recv_e, recv_w, row_n, row_s, mrow_n, mrow_s, wrow_n, wrow_s,
           sums, wp, pack, geo, coef, osem, ssem, rsem, *reduce_refs):
    lat, lon = lax.axis_index("lat"), lax.axis_index("lon")
    costs, rows, cols = w_ref.shape
    loads = [pltpu.make_async_copy(src, dst, lsem.at[i]) for i, (src, dst) in enumerate(
        zip((f_hbm, de_hbm, dn_hbm, st_hbm, mk_hbm, w_hbm),
            (f_ref, de_ref, dn_ref, st_ref, mk_ref, w_ref)))]
    for c in loads:
        c.start()

    def peer(dlat, dlon):
        return (lax.rem(lat + dlat + nlat, nlat), lax.rem(lon + dlon + nlon, nlon))

    peers = {(a % nlat, b % nlon) for a in (-1, 0, 1) for b in (-1, 0, 1)}
    peers |= {o for stage in stages for o in stage}
    peers = sorted(peers - {(0, 0)})
    barrier = pltpu.get_barrier_semaphore()
    for a, b in peers:
        pl.semaphore_signal(barrier, inc=1, device_id=peer(a, b), device_id_type=MESH)

    for c in loads:
        c.wait()

    lane = lax.broadcasted_iota(jnp.int32, (rows, 128), 1)
    wide = [f_ref, de_ref, dn_ref, st_ref, mk_ref]
    for ref, at, first in ((send_w, slice(0, 128), True), (send_e, slice(cols - 128, cols), False)):
        buf = jnp.zeros((rows, 128), jnp.float32)
        pos = 0
        for i in range(5 + costs):
            width = HC if i < 5 else HW
            tile = (wide[i][:, at] if i < 5 else w_ref[i - 5, :, at]).astype(jnp.float32)
            tile = roll(tile, pos if first else pos + width, 1)
            buf = jnp.where((lane >= pos) & (lane < pos + width), tile, buf)
            pos += width
        ref[...] = buf
    pl.semaphore_wait(barrier, len(peers))

    copies = []

    def send(src, dst, dev):
        i = len(copies)
        c = pltpu.make_async_remote_copy(src_ref=src, dst_ref=dst, send_sem=ssem.at[i],
                                         recv_sem=rsem.at[i], device_id=dev, device_id_type=MESH)
        c.start()
        copies.append(c)

    lo, hi = pl.ds(0, HR), pl.ds(rows - HR, HR)
    for src, dst, d in ((send_w, recv_e, -1), (send_e, recv_w, 1)):
        send(src.at[lo], dst.at[pl.ds(rows, HR)], peer(-1, d))
        send(src.at[hi], dst.at[pl.ds(rows + HR, HR)], peer(1, d))
        send(src, dst.at[pl.ds(0, rows)], peer(0, d))
    for i in range(5):
        src = wide[i]
        send(src.at[lo], row_n.at[i] if i < 4 else mrow_n, peer(-1, 0))
        send(src.at[hi], row_s.at[i] if i < 4 else mrow_s, peer(1, 0))
    early = len(copies)
    send(w_ref.at[:, pl.ds(0, HB)], wrow_n, peer(-1, 0))
    send(w_ref.at[:, pl.ds(rows - HB, HB)], wrow_s, peer(1, 0))
    for c in copies[:early]:
        c.wait_recv()

    full = rows + 2 * HR
    lane = lax.broadcasted_iota(jnp.int32, (full, 128), 1)
    got_e, got_w = recv_e[...], recv_w[...]

    def side(pos, width):
        a = roll(got_e, -pos, 1)
        b = roll(got_w, 128 - width - pos, 1)
        return jnp.where(lane < width, a, jnp.where(lane >= 128 - width, b, 0.0))

    def padded(i):
        if i < 4:
            top, mid, low = row_n[i], wide[i][...], row_s[i]
        else:
            top, mid, low = (r[...].astype(jnp.float32) for r in (mrow_n, mk_ref, mrow_s))
        return jnp.concatenate([jnp.concatenate([mid, top, low], axis=0), side(HC * i, HC)], axis=1)

    ringc = cols + 128
    row_id = lax.broadcasted_iota(jnp.int32, (full, ringc), 0)
    keep_n = (lat < nlat - 1).astype(jnp.float32)
    keep_s = (lat > 0).astype(jnp.float32)
    edge = jnp.where(row_id < rows, 1.0, jnp.where(row_id < rows + HR, keep_n, keep_s))
    wet = padded(4) * edge
    ex = padded(1) * wet * east(wet)
    ey = padded(2) * wet * north(wet)
    base = wet * padded(3) + 1.0 - wet
    diag = base + ex + roll(ex, 1, 1) + ey + roll(ey, 1, 0)
    rs = lax.rsqrt(diag)
    rs = rs * (1.5 - 0.5 * diag * rs * rs)
    rs_e, rs_n = rs * east(rs), rs * north(rs)
    e2 = 2.0 * ex * rs_e
    n2 = 2.0 * ey * rs_n

    def twice(v, e2, n2):
        return e2 * east(v) + roll(e2 * v, 1, 1) + n2 * north(v) + roll(n2 * v, 1, 0)

    us = [rs * padded(0)]
    us.append(0.5 * twice(us[0], e2, n2))
    for k in range(1, ITERS):
        us.append(twice(us[k], e2, n2) - us[k - 1])

    inner = [u[:rows, :cols] for u in us]
    rs_in = rs[:rows, :cols]

    def put(at, field):
        line = jnp.sum(field, axis=0, keepdims=True)
        tot = line[:, :128]
        for c in range(128, cols, 128):
            tot = tot + line[:, c:c + 128]
        sums[at:at + 1, :] = tot

    sums[...] = jnp.zeros_like(sums)
    mom = ITERS * costs
    for k in range(ITERS):
        put(mom + 2 * k, inner[k] * inner[k])
        put(mom + 2 * k + 1, inner[k] * inner[k + 1])
    for n in range(costs):
        wn = w_ref[n] * rs_in
        for k in range(ITERS):
            put(k * costs + n, wn * inner[k])
    nsum = sums.shape[0]
    lane_s = lax.broadcasted_iota(jnp.int32, (nsum, 128), 1)
    row_s_id = lax.broadcasted_iota(jnp.int32, (nsum, 128), 0)
    by_row = jnp.sum(sums[...], axis=1, keepdims=True)
    mine = jnp.sum(jnp.where(lane_s == row_s_id, by_row, 0.0), axis=0, keepdims=True)
    reduce_copies = []

    def start(stage, value):
        mailbox, got, ss, rv = reduce_refs[4 * stage:4 * stage + 4]
        mailbox[...] = value
        group = []
        for i, (a, b) in enumerate(stages[stage]):
            c = pltpu.make_async_remote_copy(src_ref=mailbox, dst_ref=got.at[i], send_sem=ss.at[i],
                                             recv_sem=rv.at[i], device_id=peer(a, b),
                                             device_id_type=MESH)
            c.start()
            group.append(c)
        reduce_copies.extend(group)
        return group

    def finish(stage, group, value):
        for c in group:
            c.wait_recv()
        for i in range(len(group)):
            value = value + reduce_refs[4 * stage + 1][i]
        return value

    group = start(0, mine)

    for c in copies[early:]:
        c.wait_recv()

    def cut(x):
        return jnp.concatenate([x[:rows + HB], x[full - HB:]], axis=0)

    rs_b = cut(rs)
    for n in range(costs):
        block = jnp.concatenate([w_ref[n], wrow_n[n], wrow_s[n]], axis=0)
        tile = cut(side(5 * HC + HW * n, HW))
        wp[n] = rs_b * jnp.concatenate([block, tile], axis=1)
    for k in range(ITERS + 1):
        pack[k] = cut(us[k])
    pack[ITERS + 1], pack[ITERS + 2], pack[ITERS + 3] = cut(e2), cut(n2), rs_b
    wet_in = wet[:rows, :cols]
    me = wet_in * east(wet)[:rows, :cols]
    mn = wet_in * north(wet)[:rows, :cols]
    geo[0], geo[1] = me, mn
    geo[2] = 2.0 * me * rs_e[:rows, :cols]
    geo[3] = 2.0 * mn * rs_n[:rows, :cols]
    saves = [pltpu.make_async_copy(src, dst, osem.at[i]) for i, (src, dst) in enumerate(
        ((pack, pack_out), (geo, geo_out), (wp, wp_out), (coef, coef_out)))]
    for c in saves[:3]:
        c.start()

    total = finish(0, group, mine)
    for stage in range(1, len(stages)):
        total = finish(stage, start(stage, total), total)

    tot8 = jnp.broadcast_to(total, (costs, 128))
    lane8 = lax.broadcasted_iota(jnp.int32, (costs, 128), 1)
    sub8 = lax.broadcasted_iota(jnp.int32, (costs, 128), 0)

    def pick(index):
        return jnp.broadcast_to(
            jnp.sum(jnp.where(lane8 == index, tot8, 0.0), axis=1, keepdims=True), (costs, 128))

    proj = [pick(k * costs + sub8) for k in range(ITERS)]
    raw = [pick(mom + m) for m in range(2 * ITERS)]
    mu = [raw[0], raw[1]]
    for k in range(1, ITERS):
        mu += [2.0 * raw[2 * k] - raw[0], 2.0 * raw[2 * k + 1] - raw[1]]
    cost, pull = jax.vjp(cost_of, mu, proj)
    mu_bar, x = pull(jnp.ones_like(cost))
    even = [2.0 * mu_bar[2 * k] for k in range(ITERS)]
    odd = [2.0 * mu_bar[2 * k + 1] for k in range(ITERS)]
    even[0] = mu_bar[0] - 0.5 * sum(even[1:])
    odd[0] = mu_bar[1] - 0.5 * sum(odd[1:])
    for k in range(ITERS):
        coef[3 * k], coef[3 * k + 1], coef[3 * k + 2] = x[k], 2.0 * even[k], odd[k]
    saves[3].start()
    for c in copies + reduce_copies:
        c.wait_send()
    for c in saves:
        c.wait()


def adjoint_kernel(wp_hbm, pack_hbm, geo_hbm, coef_hbm, fa_hbm, ge_hbm, gn_hbm,
                   wp, pack, geo, coef, u_in, u_east, u_north, quad, fa_ref, ge_ref, gn_ref,
                   lsem, wsem, osem):
    costs, rows, cols = fa_ref.shape
    ringc = wp.shape[2]
    loads = [pltpu.make_async_copy(src, dst, lsem.at[i]) for i, (src, dst) in enumerate(
        ((pack_hbm, pack), (coef_hbm, coef), (geo_hbm, geo)))]
    for c in loads:
        c.start()

    def weight(n):
        return pltpu.make_async_copy(wp_hbm.at[n], wp.at[n], wsem.at[n])

    def results(n):
        return [pltpu.make_async_copy(src.at[n], dst.at[n], osem.at[i, n])
                for i, (src, dst) in enumerate(((fa_ref, fa_hbm), (ge_ref, ge_hbm), (gn_ref, gn_hbm)))]

    for n in range(costs):
        weight(n).start()
    for c in loads:
        c.wait()
    for k in range(ITERS):
        u = pack[k] if k else 0.5 * pack[0]
        u_in[k] = u[:rows, :cols]
        u_east[k] = east(u)[:rows, :cols]
        u_north[k] = north(u)[:rows, :cols]
        quad[k] = pack[k] + pack[k - 2] if k > 1 else pack[k]
    quad[ITERS] = 0.5 * pack[ITERS] + pack[ITERS - 2]

    def one(n, carry):
        def c(i):
            return jnp.concatenate([coef[i, pl.ds(n, 1), :]] * (ringc // 128), axis=1)

        weight(n).wait()
        wn = wp[n]
        ub = [pack.at[k] for k in range(ITERS + 1)]
        e2b, n2b = pack[ITERS + 1], pack[ITERS + 2]
        nxt = c(3 * ITERS - 1) * ub[ITERS - 1][...]
        nxt2 = None
        dd = nxt * quad[ITERS]
        eb = nb = du = None
        for k in range(ITERS - 1, -1, -1):
            le, ln = east(nxt), north(nxt)
            s2 = e2b * le + roll(e2b * nxt, 1, 1) + n2b * ln + roll(n2b * nxt, 1, 0)
            if k == 0:
                s2 = 0.5 * s2
            lin = nxt[:rows, :cols]
            ea = lin * u_east[k] + le[:rows, :cols] * u_in[k]
            na = lin * u_north[k] + ln[:rows, :cols] * u_in[k]
            eb = ea if eb is None else eb + ea
            nb = na if nb is None else nb + na
            seed = c(3 * k + 1) * ub[k][...] + c(3 * k + 2) * ub[k + 1][...]
            if k > 0:
                seed = seed + c(3 * k - 1) * ub[k - 1][...]
            lam = c(3 * k) * wn + seed + s2
            if nxt2 is not None:
                lam = lam - nxt2
            dd = dd + lam * quad[k]
            du = seed * ub[k][...] if du is None else du + seed * ub[k][...]
            nxt, nxt2 = lam, nxt
        rs = pack[ITERS + 3]
        fa_ref[n] = rs[:rows, :cols] * nxt[:rows, :cols]
        db = -(rs * rs) * (dd - 0.5 * du)
        db_in = db[:rows, :cols]
        ge_ref[n] = geo[2] * eb + geo[0] * (db_in + east(db)[:rows, :cols])
        gn_ref[n] = geo[3] * nb + geo[1] * (db_in + north(db)[:rows, :cols])
        for r in results(n):
            r.start()
        return carry

    lax.fori_loop(0, costs, one, 0)
    for n in range(costs):
        for r in results(n):
            r.wait()


def solution(mesh):
    nlat, nlon = mesh.shape["lat"], mesh.shape["lon"]

    def body(forcing, depth_east, depth_north, surface_term, ocean_mask, cost_weights):
        costs, rows, cols = cost_weights.shape
        full, ringc = rows + 2 * HR, cols + 128
        f32 = jnp.float32
        dma = pltpu.SemaphoreType.DMA
        nsum = -(-(ITERS * costs + 2 * ITERS) // 8) * 8
        every = [(a, b) for a in range(nlat) for b in range(nlon) if a or b]
        stages = [every] if len(every) < 64 else [
            [(0, b) for b in range(1, nlon)], [(a, 0) for a in range(1, nlat)]]
        reduce_scratch = [
            ref for g in stages for ref in (
                pltpu.VMEM((1, 128), f32), pltpu.VMEM((len(g), 1, 128), f32),
                dma((len(g),)), dma((len(g),)))]
        bf = rows + 2 * HB
        shapes = ((costs, bf, ringc), (ITERS + 4, bf, ringc), (4, rows, cols), (3 * ITERS, costs, 128))
        hbm = pl.BlockSpec(memory_space=pltpu.HBM)
        mids = pl.pallas_call(
            functools.partial(kernel, nlat, nlon, stages),
            out_shape=[jax.ShapeDtypeStruct(x, f32) for x in shapes],
            in_specs=[hbm] * 6,
            out_specs=[hbm] * 4,
            scratch_shapes=[
                *[pltpu.VMEM((rows, cols), f32)] * 4,
                pltpu.VMEM((rows, cols), jnp.int32),
                pltpu.VMEM((costs, rows, cols), f32),
                dma((6,)),
                pltpu.VMEM((rows, 128), f32),
                pltpu.VMEM((rows, 128), f32),
                pltpu.VMEM((full, 128), f32),
                pltpu.VMEM((full, 128), f32),
                pltpu.VMEM((4, HR, cols), f32),
                pltpu.VMEM((4, HR, cols), f32),
                pltpu.VMEM((HR, cols), jnp.int32),
                pltpu.VMEM((HR, cols), jnp.int32),
                pltpu.VMEM((costs, HB, cols), f32),
                pltpu.VMEM((costs, HB, cols), f32),
                pltpu.VMEM((nsum, 128), f32),
                *[pltpu.VMEM(x, f32) for x in shapes],
                dma((4,)),
                dma((18,)),
                dma((18,)),
                *reduce_scratch,
            ],
            compiler_params=pltpu.CompilerParams(
                collective_id=0, has_side_effects=True, vmem_limit_bytes=63 * 1024 * 1024
            ),
        )(forcing, depth_east, depth_north, surface_term, ocean_mask, cost_weights)
        out = (costs, rows, cols)
        return pl.pallas_call(
            adjoint_kernel,
            out_shape=[jax.ShapeDtypeStruct(out, f32)] * 3,
            in_specs=[hbm] * 4,
            out_specs=[hbm] * 3,
            scratch_shapes=[
                *[pltpu.VMEM(x, f32) for x in shapes],
                *[pltpu.VMEM((ITERS, rows, cols), f32)] * 3,
                pltpu.VMEM((ITERS + 1, bf, ringc), f32),
                *[pltpu.VMEM(out, f32)] * 3,
                dma((3,)),
                dma((costs,)),
                dma((3, costs)),
            ],
            compiler_params=pltpu.CompilerParams(vmem_limit_bytes=63 * 1024 * 1024),
        )(*mids)

    grid = P("lat", "lon")
    field = P(None, "lat", "lon")
    return jax.shard_map(
        body,
        mesh=mesh,
        in_specs=(grid, grid, grid, grid, grid, field),
        out_specs=(field, field, field),
        check_vma=False,
    )
```
